32 devices in a mesh: comp: 2 (over x), rows: 4 (over z), cols: 4 (over y, core).
Axes of the slice: x: 2, y: 2, z: 4, core: 2. Of those that a mesh axis runs over, the one named last changes fastest.
Arguments:
- atm_state: float32 [4, 4, 256, 512], P(None, None, ('comp', 'rows'), 'cols'), may hold values from -6 to 6
- ocean_state: float32 [4, 8, 128, 512], P(None, None, ('comp', 'rows'), 'cols'), may hold values from -6 to 6
- coupling: float32 [256, 512], P(('comp', 'rows'), 'cols'), may hold values from 0.2 to 2
- down_weights: bfloat16 [8, 128, 128, 128], P(('comp', 'rows'), 'cols'), may hold values from -0.5 to 0.5
- down_src: int32 [8, 128], P(('comp', 'rows'), 'cols'), may hold values from 0 to 31
- down_row: int32 [8, 128], P(('comp', 'rows'), 'cols'), may hold values from 0 to 3, as said below
- down_blk: int32 [8, 128], P(('comp', 'rows'), 'cols'), may hold values from 0 to 15
- up_weights: bfloat16 [8, 128, 128, 128], P(('comp', 'rows'), 'cols'), may hold values from -0.5 to 0.5
- up_dst: int32 [8, 128], P(('comp', 'rows'), 'cols'), may hold values from 0 to 31
- up_src: int32 [8, 128], P(('comp', 'rows'), 'cols'), may hold values from 0 to 63, as said below
Outputs:
- atm_out: float32 [4, 4, 256, 512], P(None, None, ('comp', 'rows'), 'cols')
- ocean_out: float32 [4, 8, 128, 512], P(None, None, ('comp', 'rows'), 'cols')
The draws below stay inside these ranges and needn't reach their ends.
Inputs may be any that keep to these rules, and one draw needn't show every extreme that they name: `down_row`: among one device's 32 down entries, no rows index is named more than 16 times, and some rows index exactly 16 times. `up_src`: no two of one device's 32 up entries name the same value; at most 16 of them come from one rows index, and exactly 16 from some rows index.
All inputs are finite; a program needn't handle non-finite values.
Results may differ from the reference program's by a relative error of at most 0.0003.
Values sent between devices are 32-bit elements; how exact they have to be, the bound alone decides.
A program may use at most 64 MiB of HBM per device.

```python
import math
import jax
import jax.numpy as jnp
import numpy as np
from jax import lax

NF = 4
NP = 4
ALEV = 4
OXD = 16
OYD = 128
OLEV = 8
BLK = 128
NBLK = 32
AXD = 32
AYD = 128
ABLK = 32
OBLK = 16
SLOT = 16
PARTITION_SETS = 8
AX = 256
AY = 512
OX = 128
OY = 512
N_ROWS = 4
N_COLS = 4


def pick_rows(key):
    contender_total = N_ROWS * SLOT
    contender_partition = jnp.arange(contender_total)
    holder_partition = contender_partition // SLOT
    extra_credit_seed, primary_sort_measure, perturbation_seed, sequence_sort_measure = jax.random.split(key, 4)
    extra_credit_value = jax.random.randint(extra_credit_seed, (PARTITION_SETS, N_COLS, N_ROWS), 0, 4)
    favoured_partition = jax.random.randint(primary_sort_measure, (PARTITION_SETS, N_COLS, 1), 0, N_ROWS)
    extra_credit_value = jnp.where(jnp.arange(N_ROWS) == favoured_partition, 8, extra_credit_value)
    stochastic_perturbation = jax.random.randint(perturbation_seed, (PARTITION_SETS, N_COLS, contender_total), 0, 1024)
    priority_merit = (jnp.take(extra_credit_value, holder_partition, axis=2) * 1024 + stochastic_perturbation) * contender_total + contender_partition
    ignored, chosen = lax.top_k(priority_merit, NBLK)
    order = jax.random.randint(sequence_sort_measure, (PARTITION_SETS, N_COLS, NBLK), 0, 1 << 20) * NBLK + jnp.arange(NBLK)
    shuffle = jnp.argsort(order, axis=-1)
    return jnp.take_along_axis(chosen, shuffle, axis=-1)


def up_requests(key):
    chosen = pick_rows(jax.random.fold_in(key, 23))
    source_row = chosen // SLOT
    slot_index = chosen % SLOT
    order = jax.random.randint(jax.random.fold_in(key, 29), (PARTITION_SETS, N_COLS, N_ROWS, OBLK), 0, 1 << 20) * OBLK + jnp.arange(OBLK)
    shuffles = jnp.argsort(order, axis=-1)
    per_entry = jnp.take_along_axis(shuffles, source_row[..., None], axis=2)
    blocks = jnp.take_along_axis(per_entry, slot_index[..., None], axis=3)[..., 0]
    return (source_row * OBLK + blocks).astype(jnp.int32)


def draw_down_row(key, part):
    chosen = pick_rows(jax.random.fold_in(key, 11))
    return (chosen // SLOT).reshape(PARTITION_SETS, N_COLS * NBLK).astype(jnp.int32)


def draw_up_src(key, part):
    return up_requests(key).reshape(PARTITION_SETS, N_COLS * NBLK)


def place_ends(values, key, smallest, high):
    longest = values.shape.index(max(values.shape))
    spots = []
    for shift in (0, 1):
        where = [jax.random.randint(jax.random.fold_in(key, axis), (), 0, length) for axis, length in enumerate(values.shape)]
        where[longest] = (where[longest] + shift) % values.shape[longest]
        spots.append(tuple(where))
    return values.at[spots[0]].set(smallest).at[spots[1]].set(high)


def steps_of(own_key, extent, shards, low, largest):
    def one(dim, parts):
        draws = jax.random.uniform(jax.random.fold_in(jax.random.fold_in(own_key, 6), dim), (parts,), jnp.float32, low / len(shards), largest / len(shards))
        return jnp.repeat(jnp.exp(draws), extent[dim] // parts).reshape((-1,) + (1,) * (len(extent) - dim - 1))

    gain = one(*shards[0])
    for cut in shards[1:]:
        gain = gain * one(*cut)
    return gain


def gaussian(own_key, extent, spread, bound, pieces=(), dtype=jnp.bfloat16):
    level = steps_of(own_key, extent, pieces, -0.22, 0.18) if pieces else 1.0
    result = jax.random.normal(own_key, extent, jnp.float32) * spread * level
    return jnp.minimum(jnp.maximum(result, -bound), bound).astype(dtype)


def setup_inputs(seed: int = 0) -> dict:
    keys = jax.random.split(jax.random.key(seed), 11)
    return {
        "atm_state": gaussian(keys[0], (NF, ALEV, AX, AY), 1.0, 6.0, ((2, 8), (3, 4)), jnp.float32),
        "ocean_state": gaussian(keys[1], (NF, OLEV, OX, OY), 1.0, 6.0, ((2, 8), (3, 4)), jnp.float32),
        "coupling": jnp.clip(jnp.exp(math.log(2.0) - 2.3025851 * jax.random.uniform(keys[2], (AX, AY), jnp.float32) ** steps_of(keys[2], (AX, AY), ((0, 8), (1, 4)), -0.2, 0.2)), 0.2, 2.0),
        "down_weights": gaussian(keys[3], (PARTITION_SETS, N_COLS * NBLK, BLK, BLK), BLK ** -0.5, 0.5, ((0, 8), (1, 4))),
        "down_src": place_ends(jax.random.randint(keys[4], (PARTITION_SETS, N_COLS * NBLK), 0, ABLK), jax.random.fold_in(keys[4], 1), 0, ABLK - 1).astype(jnp.int32),
        "down_row": draw_down_row(jax.random.fold_in(keys[10], 71), 0),
        "down_blk": place_ends(jax.random.randint(keys[6], (PARTITION_SETS, N_COLS * NBLK), 0, OBLK), jax.random.fold_in(keys[6], 1), 0, OBLK - 1).astype(jnp.int32),
        "up_weights": gaussian(keys[7], (PARTITION_SETS, N_COLS * NBLK, BLK, BLK), BLK ** -0.5, 0.5, ((0, 8), (1, 4))),
        "up_dst": place_ends(jax.random.randint(keys[8], (PARTITION_SETS, N_COLS * NBLK), 0, ABLK), jax.random.fold_in(keys[8], 1), 0, ABLK - 1).astype(jnp.int32),
        "up_src": draw_up_src(jax.random.fold_in(keys[10], 71), 0),
    }


EXACT = lax.Precision.HIGHEST
VISCOSITY = 0.01
ATM_GAIN = 0.5
DIFFUSION = 0.1
SEA_GAIN = 0.5

def gll_second():
    gll_nodes = np.array([-1.0, -1.0 / np.sqrt(5.0), 1.0 / np.sqrt(5.0), 1.0])
    npoints = gll_nodes.shape[0]
    bary_weights = np.array([1.0 / np.prod([gll_nodes[col_idx] - gll_nodes[other] for other in range(npoints) if other != col_idx]) for col_idx in range(npoints)])
    derivative = np.zeros((npoints, npoints))
    for row_idx in range(npoints):
        for col_idx in range(npoints):
            if row_idx != col_idx:
                derivative[row_idx, col_idx] = bary_weights[col_idx] / bary_weights[row_idx] / (gll_nodes[row_idx] - gll_nodes[col_idx])
        derivative[row_idx, row_idx] = -np.sum(derivative[row_idx])
    return (derivative @ derivative).astype(np.float32)

def pair_average(field, dim_index):
    length = field.shape[dim_index]
    lower = jnp.roll(field, 1, dim_index)
    upper = jnp.roll(field, -1, dim_index)
    bcast_shape = [1] * field.ndim
    bcast_shape[dim_index] = length
    position = (jnp.arange(length) % NP).reshape(bcast_shape)
    return jnp.where(position == 0, (field + lower) * 0.5, jnp.where(position == NP - 1, (field + upper) * 0.5, field))

def local_laplacian(field):
    second = jnp.asarray(gll_second())
    fields, levels, x_len, y_len = field.shape
    along_x = field.reshape(fields, levels, x_len // NP, NP, y_len)
    diff_x = jnp.einsum('ij,flejy->fleiy', second, along_x, precision=EXACT).reshape(field.shape)
    along_y = field.reshape(fields, levels, x_len, y_len // NP, NP)
    diff_y = jnp.einsum('ij,flxej->flxei', second, along_y, precision=EXACT).reshape(field.shape)
    return diff_x + diff_y

def to_blocks(field, x_cells, y_cells):
    shaped = field.reshape(NF, PARTITION_SETS, x_cells, N_COLS, y_cells).transpose(1, 3, 0, 2, 4)
    return shaped.reshape(PARTITION_SETS, N_COLS, NF, x_cells * y_cells // BLK, BLK)

def from_blocks(blocks, x_cells, y_cells):
    shaped = blocks.reshape(PARTITION_SETS, N_COLS, NF, x_cells, y_cells).transpose(2, 0, 3, 1, 4)
    return shaped.reshape(NF, PARTITION_SETS * x_cells, N_COLS * y_cells)

def reference(atm_state, ocean_state, coupling, down_weights, down_src, down_row, down_blk, up_weights, up_dst, up_src):
    surface = to_blocks(ocean_state[:, 0], OXD, OYD)
    sources = up_src.reshape(PARTITION_SETS, N_COLS, NBLK)
    comp_first = (jnp.arange(PARTITION_SETS) // N_ROWS * N_ROWS)[:, None, None]
    column = jnp.arange(N_COLS)[None, :, None]
    picked = surface[comp_first + sources // OBLK, column, :, sources % OBLK]
    w_up = up_weights.astype(jnp.float32).reshape(PARTITION_SETS, N_COLS, NBLK, BLK, BLK)
    remapped = jnp.einsum('gkbij,gkbfj->gkbfi', w_up, picked, precision=EXACT)
    to_atm = (up_dst.reshape(PARTITION_SETS, N_COLS, NBLK)[..., None] == jnp.arange(ABLK)).astype(jnp.float32)
    sea_blocks = jnp.einsum('gkba,gkbfi->gkfai', to_atm, remapped, precision=EXACT)
    sea_at_atm = from_blocks(sea_blocks, AXD, AYD)
    flux_atm = coupling * (sea_at_atm - atm_state[:, -1])
    flux_blocks = to_blocks(flux_atm, AXD, AYD)
    group_index = jnp.arange(PARTITION_SETS)[:, None, None]
    down_sources = down_src.reshape(PARTITION_SETS, N_COLS, NBLK)
    chosen = flux_blocks[group_index, column, :, down_sources]
    w_down = down_weights.astype(jnp.float32).reshape(PARTITION_SETS, N_COLS, NBLK, BLK, BLK)
    partial_value = jnp.einsum('gkbij,gkbfj->gkbfi', w_down, chosen, precision=EXACT)
    dest_group = comp_first + down_row.reshape(PARTITION_SETS, N_COLS, NBLK)
    dest_block = down_blk.reshape(PARTITION_SETS, N_COLS, NBLK)
    ocean_blocks = jnp.zeros((PARTITION_SETS, N_COLS, NF, OBLK, BLK), jnp.float32)
    ocean_blocks = ocean_blocks.at[dest_group, column, :, dest_block].add(partial_value)
    flux_sea = from_blocks(ocean_blocks, OXD, OYD)
    updated = atm_state + VISCOSITY * local_laplacian(atm_state)
    updated = updated.at[:, -1].add(ATM_GAIN * flux_atm)
    atm_out = pair_average(pair_average(updated, 2), 3)
    padded = jnp.pad(ocean_state, ((0, 0), (0, 0), (1, 1), (1, 1)))
    stencil = padded[:, :, 2:, 1:-1] + padded[:, :, :-2, 1:-1] + padded[:, :, 1:-1, 2:] + padded[:, :, 1:-1, :-2] - 4.0 * ocean_state
    ocean_out = ocean_state + DIFFUSION * stencil
    ocean_out = ocean_out.at[:, 0].add(SEA_GAIN * flux_sea)
    return (atm_out, ocean_out)
```

```python
import functools

import jax
import jax.numpy as jnp
import numpy as np
from jax import lax
from jax.experimental import pallas as pl
from jax.experimental.pallas import tpu as pltpu
from jax.sharding import PartitionSpec as P

NP = 4
VISCOSITY = 0.01
ATM_GAIN = 0.5
DIFFUSION = 0.1
SEA_GAIN = 0.5
MESH = pl.DeviceIdType.MESH
F32 = jnp.float32
BF16 = jnp.bfloat16


def gll_second():
    gll_nodes = np.array([-1.0, -1.0 / np.sqrt(5.0), 1.0 / np.sqrt(5.0), 1.0])
    n = gll_nodes.shape[0]
    bary = np.array(
        [1.0 / np.prod([gll_nodes[c] - gll_nodes[o] for o in range(n) if o != c]) for c in range(n)]
    )
    derivative = np.zeros((n, n))
    for r in range(n):
        for c in range(n):
            if r != c:
                derivative[r, c] = bary[c] / bary[r] / (gll_nodes[r] - gll_nodes[c])
        derivative[r, r] = -np.sum(derivative[r])
    return derivative @ derivative


def iota(shape, dim):
    return lax.broadcasted_iota(jnp.int32, shape, dim)


def bits(n):
    assert n & (n - 1) == 0
    return n.bit_length() - 1


def split(x):
    hi = x.astype(BF16)
    return hi, (x - hi.astype(F32)).astype(BF16)


def dot(a, b):
    return jnp.dot(a, b, preferred_element_type=F32)


def dot_t(a, b):
    return lax.dot_general(a, b, (((1,), (1,)), ((), ())), preferred_element_type=F32)


def kernel(
    sizes,
    atm, oce, coup, dw, dsrc, drow, dblk, uw, udst, usrc,
    aout, oout,
    av, ov, cv, dwv, uwv, in_sem,
    land, land_s, land_r,
    oxs, oxr, oys, oyr, axs, axr, ays, ayr, fxs, fxr, fys, fyr, halo_s, halo_r,
    dns, dnr, dn_s, dn_r,
    ub, aov, oov, flb, sel_u, t_u, sel_d, t_d, picked, rem, out_sem,
):
    comps, rows, cols = sizes
    c = lax.axis_index("comp")
    r = lax.axis_index("rows")
    k = lax.axis_index("cols")
    nf, al, ax, ln = av.shape
    ol, ox = ov.shape[1], ov.shape[2]
    nb = dsrc.shape[1]
    group = 2 * nf
    ent = nb * group
    total = comps * rows
    g = c * rows + r

    ins = [
        pltpu.make_async_copy(oce, ov, in_sem.at[0]),
        pltpu.make_async_copy(atm, av, in_sem.at[1]),
        pltpu.make_async_copy(coup, cv, in_sem.at[2]),
        pltpu.make_async_copy(uw.at[0], uwv, in_sem.at[3]),
        pltpu.make_async_copy(dw.at[0], dwv, in_sem.at[4]),
    ]
    for copy in ins:
        copy.start()

    def x_neighbour(step):
        other = lax.rem(g + step + total, total)
        return {"comp": other // rows, "rows": lax.rem(other, rows)}

    def y_neighbour(step):
        return {"cols": lax.rem(k + step + cols, cols)}

    def row_peer(step):
        return {"rows": lax.rem(r + step, rows)}

    partners = [x_neighbour(-1), x_neighbour(1), y_neighbour(-1), y_neighbour(1)]
    partners += [row_peer(d) for d in range(1, rows)]
    barrier = pltpu.get_barrier_semaphore()
    for who in partners:
        pl.semaphore_signal(barrier, inc=1, device_id=who, device_id_type=MESH)

    lane = iota((1, ln), 1)

    ins[0].wait()
    west = jnp.zeros((ox, ln), F32)
    east = jnp.zeros((ox, ln), F32)
    for f in range(nf):
        for l in range(ol):
            q = f * ol + l
            tile = ov[f, l]
            oxs[0, q : q + 1, :] = tile[0:1, :]
            oxs[1, q : q + 1, :] = tile[ox - 1 : ox, :]
            west = jnp.where(lane == q, tile[:, 0:1], west)
            east = jnp.where(lane == q, tile[:, ln - 1 : ln], east)
    oys[0] = west
    oys[1] = east

    pl.semaphore_wait(barrier, len(partners))

    def send(src, dst, s_sem, r_sem, who):
        copy = pltpu.make_async_remote_copy(
            src_ref=src, dst_ref=dst, send_sem=s_sem, recv_sem=r_sem,
            device_id=who, device_id_type=MESH,
        )
        copy.start()
        return copy

    def exchange(which, src, dst, neighbour):
        return [
            send(src.at[i], dst.at[i], halo_s.at[which, i], halo_r.at[which, i], neighbour(step))
            for i, step in enumerate((-1, 1))
        ]

    order = sorted(range(1, rows), key=lambda d: -min(d, rows - d))
    surface = [
        send(ov.at[:, 0], land.at[d], land_s.at[d], land_r.at[d], row_peer(d)) for d in order
    ]
    sea_x = exchange(0, oxs, oxr, x_neighbour)
    sea_y = exchange(1, oys, oyr, y_neighbour)
    land[0] = ov[:, 0]

    second = gll_second() * VISCOSITY

    def coefficient(position, d):
        out = jnp.zeros(position.shape, F32)
        for i in range(NP):
            if 0 <= i + d < NP:
                out = jnp.where(position == i, float(second[i, i + d]), out)
        return out

    px = iota((8, ln), 0) & (NP - 1)
    py = iota((8, ln), 1) & (NP - 1)
    here = 1.0 + coefficient(px, 0) + coefficient(py, 0)
    steps = [d for d in range(1 - NP, NP) if d]
    cx = {d: coefficient(px, d) for d in steps}
    cy = {d: coefficient(py, d) for d in steps}
    ins[1].wait()
    for f in range(nf):
        for l in range(al):
            q = f * al + l
            for t in range(ax // 8):
                a = av[f, l, 8 * t : 8 * t + 8, :]
                u = here * a
                for d in steps:
                    u += cx[d] * pltpu.roll(a, (-d) % 8, 0)
                    u += cy[d] * pltpu.roll(a, (-d) % ln, 1)
                ub[q, 8 * t : 8 * t + 8, :] = u
                if t == 0:
                    axs[0, q : q + 1, :] = u[0:1, :]
                if t == ax // 8 - 1:
                    axs[1, q : q + 1, :] = u[7:8, :]
    atm_x = exchange(2, axs, axr, x_neighbour)

    def column(ref):
        row = ref[...].astype(F32)
        pick = (iota((ent, nb), 0) >> bits(group)) == iota((ent, nb), 1)
        return jnp.sum(jnp.where(pick, row, 0.0), axis=1, keepdims=True)

    def spread(ref):
        row = ref[...].astype(F32)
        pick = iota((nb, nb), 0) == iota((nb, nb), 1)
        col = jnp.sum(jnp.where(pick, row, 0.0), axis=1, keepdims=True)
        pick = (iota((nb, ent), 1) >> bits(group)) == iota((nb, ent), 0)
        return jnp.sum(jnp.where(pick, col, 0.0), axis=0, keepdims=True)

    def hot(a, b):
        return jnp.where(a == b, 1.0, 0.0).astype(BF16)

    me = r.astype(F32)
    part = iota((ent, 1), 0) & (group - 1)
    part_field = (part & (nf - 1)).astype(F32)
    part_low = (part >> bits(nf)).astype(F32)
    lane_field = (iota((1, ent), 1) & (nf - 1)).astype(F32)

    s = column(usrc)
    owner = jnp.floor(s * (1.0 / ox))
    slot = me - owner
    slot = jnp.where(slot < 0.0, slot + rows, slot)
    key = ((part_low * rows + slot) * nf + part_field) * ox + (s - owner * ox)
    sel_u[...] = hot(key, iota(sel_u.shape, 1).astype(F32))
    t_u[...] = hot(iota(t_u.shape, 0).astype(F32), lane_field * ax + spread(udst))
    key = (part_low * nf + part_field) * ax + column(dsrc)
    sel_d[...] = hot(key, iota(sel_d.shape, 1).astype(F32))
    slot = spread(drow) - me
    slot = jnp.where(slot < 0.0, slot + rows, slot)
    key = (slot * nf + lane_field) * ox + spread(dblk)
    t_d[...] = hot(iota(t_d.shape, 0).astype(F32), key)

    def remap(sel, source, weights, place):
        hi, lo = split(source)
        picked[...] = dot(sel[...], jnp.concatenate([hi, lo], axis=0))
        for b in range(nb):
            rows_b = slice(b * group, (b + 1) * group)
            rem[rows_b, :] = dot_t(picked[rows_b, :].astype(BF16), weights[b])
        hi, lo = split(rem[...])
        both = dot(place[...], jnp.concatenate([hi, lo], axis=1))
        return both[:, :ln] + both[:, ln:]

    ins[2].wait()
    ins[3].wait()
    for copy in surface:
        copy.wait_recv()
    sea = remap(sel_u, land[...].reshape(rows * nf * ox, ln), uwv, t_u)
    flux = cv[...] * (sea.reshape(nf, ax, ln) - av[:, al - 1])
    flb[...] = flux
    for f in range(nf):
        fxs[0, f : f + 1, :] = flb[f, 0:1, :]
        fxs[1, f : f + 1, :] = flb[f, ax - 1 : ax, :]
    flux_x = exchange(4, fxs, fxr, x_neighbour)

    ins[4].wait()
    down = remap(sel_d, flb[...].reshape(nf * ax, ln), dwv, t_d)
    dns[...] = down.reshape(rows, nf, ox, ln)
    going = [send(dns.at[d], dnr.at[d], dn_s.at[d], dn_r.at[d], row_peer(d)) for d in order]

    row_id = iota((ax, ln), 0)
    lane_id = iota((ax, ln), 1)
    first_row, last_row = row_id == 0, row_id == ax - 1
    first_lane, last_lane = lane_id == 0, lane_id == ln - 1
    x_pos, y_pos = row_id & (NP - 1), lane_id & (NP - 1)

    def average(u, axis, before, after):
        first, last, pos = (
            (first_row, last_row, x_pos) if axis == 0 else (first_lane, last_lane, y_pos)
        )
        low = jnp.where(first, before, pltpu.roll(u, 1, axis))
        high = jnp.where(last, after, pltpu.roll(u, u.shape[axis] - 1, axis))
        return jnp.where(
            pos == 0, (u + low) * 0.5, jnp.where(pos == NP - 1, (u + high) * 0.5, u)
        )

    def x_pass(copies, recv, store, packed, count):
        for copy in copies:
            copy.wait_recv()
        west = jnp.zeros((ax, ln), F32)
        east = jnp.zeros((ax, ln), F32)
        for q in range(count):
            e = average(store[q], 0, recv[1, q : q + 1, :], recv[0, q : q + 1, :])
            store[q] = e
            west = jnp.where(lane == q, e[:, 0:1], west)
            east = jnp.where(lane == q, e[:, ln - 1 : ln], east)
        packed[0] = west
        packed[1] = east

    x_pass(atm_x, axr, ub, ays, nf * al)
    atm_y = exchange(3, ays, ayr, y_neighbour)

    for copy in sea_x + sea_y:
        copy.wait_recv()
    o_row = iota((ox, ln), 0)
    o_lane = iota((ox, ln), 1)
    west = jnp.where(k == 0, 0.0, oyr[1])
    east = jnp.where(k == cols - 1, 0.0, oyr[0])

    def stencil(f, l):
        q = f * ol + l
        x = ov[f, l]
        before = jnp.where(g == 0, 0.0, oxr[1, q : q + 1, :])
        after = jnp.where(g == total - 1, 0.0, oxr[0, q : q + 1, :])
        ring = jnp.where(o_row == 0, before, pltpu.roll(x, 1, 0))
        ring += jnp.where(o_row == ox - 1, after, pltpu.roll(x, ox - 1, 0))
        ring += jnp.where(o_lane == 0, west[:, q : q + 1], pltpu.roll(x, 1, 1))
        ring += jnp.where(o_lane == ln - 1, east[:, q : q + 1], pltpu.roll(x, ln - 1, 1))
        oov[f, l] = x + DIFFUSION * (ring - 4.0 * x)

    for f in range(nf):
        for l in range(ol):
            stencil(f, l)
    outs = [pltpu.make_async_copy(oov.at[:, 1:], oout.at[:, 1:], out_sem.at[0])]
    outs[0].start()

    x_pass(flux_x, fxr, flb, fys, nf)
    flux_y = exchange(5, fys, fyr, y_neighbour)

    for copy in atm_y:
        copy.wait_recv()
    before, after = ayr[1], ayr[0]
    for f in range(nf):
        for l in range(al):
            q = f * al + l
            aov[f, l] = average(ub[q], 1, before[:, q : q + 1], after[:, q : q + 1])
    outs.append(pltpu.make_async_copy(aov.at[:, : al - 1], aout.at[:, : al - 1], out_sem.at[1]))
    outs[1].start()

    for copy in flux_y:
        copy.wait_recv()
    before, after = fyr[1], fyr[0]
    for f in range(nf):
        e = average(flb[f], 1, before[:, f : f + 1], after[:, f : f + 1])
        aov[f, al - 1] = aov[f, al - 1] + ATM_GAIN * e
    outs.append(pltpu.make_async_copy(aov.at[:, al - 1], aout.at[:, al - 1], out_sem.at[2]))
    outs[2].start()

    for copy in going:
        copy.wait_recv()
    arrived = dns[0]
    for d in range(1, rows):
        arrived += dnr[d]
    oov[:, 0] = oov[:, 0] + SEA_GAIN * arrived
    outs.append(pltpu.make_async_copy(oov.at[:, 0], oout.at[:, 0], out_sem.at[3]))
    outs[3].start()

    for copy in surface + sea_x + sea_y + atm_x + atm_y + flux_x + flux_y + going:
        copy.wait_send()
    for copy in outs:
        copy.wait()


def body(sizes, atm, oce, coup, dw, dsrc, drow, dblk, uw, udst, usrc):
    rows = sizes[1]
    nf, al, ax, ln = atm.shape
    ol, ox = oce.shape[1], oce.shape[2]
    nb, blk = dw.shape[1], dw.shape[2]
    assert ln == blk and oce.shape[3] == blk
    fa, fo, ent = nf * al, nf * ol, nb * 2 * nf
    assert fa <= ln and fo <= ln
    vm = pltpu.VMEM
    dma = pltpu.SemaphoreType.DMA
    pair = lambda n: [vm((2, n, ln), F32)] * 2
    scratch = [
        vm(atm.shape, F32), vm(oce.shape, F32), vm(coup.shape, F32),
        vm((nb, blk, blk), BF16), vm((nb, blk, blk), BF16), dma((5,)),
        vm((rows, nf, ox, ln), F32), dma((rows,)), dma((rows,)),
        *pair(fo), *pair(ox), *pair(fa), *pair(ax), *pair(nf), *pair(ax),
        dma((6, 2)), dma((6, 2)),
        vm((rows, nf, ox, ln), F32), vm((rows, nf, ox, ln), F32), dma((rows,)), dma((rows,)),
        vm((fa, ax, ln), F32), vm(atm.shape, F32), vm(oce.shape, F32), vm((nf, ax, ln), F32),
        vm((ent, 2 * rows * nf * ox), BF16), vm((nf * ax, ent), BF16),
        vm((ent, 2 * nf * ax), BF16), vm((rows * nf * ox, ent), BF16),
        vm((ent, ln), F32), vm((ent, ln), F32), dma((4,)),
    ]
    hbm = pl.BlockSpec(memory_space=pl.ANY)
    small = pl.BlockSpec(memory_space=pltpu.VMEM)
    return pl.pallas_call(
        functools.partial(kernel, sizes),
        out_shape=(
            jax.ShapeDtypeStruct(atm.shape, F32),
            jax.ShapeDtypeStruct(oce.shape, F32),
        ),
        in_specs=[hbm, hbm, hbm, hbm, small, small, small, hbm, small, small],
        out_specs=(hbm, hbm),
        scratch_shapes=scratch,
        compiler_params=pltpu.CompilerParams(collective_id=0, has_side_effects=True),
        name="coupled_step",
    )(atm, oce, coup, dw, dsrc, drow, dblk, uw, udst, usrc)


def solution(mesh):
    sizes = tuple(mesh.shape[a] for a in ("comp", "rows", "cols"))
    tiles = P(None, None, ("comp", "rows"), "cols")
    flat = P(("comp", "rows"), "cols")
    blocks = P(("comp", "rows"), "cols", None, None)
    return jax.shard_map(
        functools.partial(body, sizes),
        mesh=mesh,
        in_specs=(tiles, tiles, flat, blocks, flat, flat, flat, blocks, flat, flat),
        out_specs=(tiles, tiles),
        check_vma=False,
    )
```

```python
import functools

import jax
import jax.numpy as jnp
import numpy as np
from jax import lax
from jax.experimental import pallas as pl
from jax.experimental.pallas import tpu as pltpu
from jax.sharding import PartitionSpec as P

NP = 4
VISCOSITY = 0.01
ATM_GAIN = 0.5
DIFFUSION = 0.1
SEA_GAIN = 0.5
MESH = pl.DeviceIdType.MESH
F32 = jnp.float32
BF16 = jnp.bfloat16


def gll_second():
    gll_nodes = np.array([-1.0, -1.0 / np.sqrt(5.0), 1.0 / np.sqrt(5.0), 1.0])
    n = gll_nodes.shape[0]
    bary = np.array(
        [1.0 / np.prod([gll_nodes[c] - gll_nodes[o] for o in range(n) if o != c]) for c in range(n)]
    )
    derivative = np.zeros((n, n))
    for r in range(n):
        for c in range(n):
            if r != c:
                derivative[r, c] = bary[c] / bary[r] / (gll_nodes[r] - gll_nodes[c])
        derivative[r, r] = -np.sum(derivative[r])
    return derivative @ derivative


def iota(shape, dim):
    return lax.broadcasted_iota(jnp.int32, shape, dim)


def bits(n):
    assert n & (n - 1) == 0
    return n.bit_length() - 1


def split(x):
    hi = x.astype(BF16)
    return hi, (x - hi.astype(F32)).astype(BF16)


def dot(a, b):
    return jnp.dot(a, b, preferred_element_type=F32)


def dot_t(a, b):
    return lax.dot_general(a, b, (((1,), (1,)), ((), ())), preferred_element_type=F32)


def kernel(
    sizes,
    atm, oce, coup, dw, dsrc_h, drow_h, dblk_h, uw, udst_h, usrc_h,
    aov, oov,
    av, ov, cv, dwv, uwv, in_sem, usrc, udst, dsrc, drow, dblk,
    land, land_s, land_r,
    oxs, oxr, oys, oyr, axs, axr, ays, ayr, fxs, fxr, fys, fyr, halo_s, halo_r,
    dns, dnr, dn_s, dn_r,
    ub, flb, sel_u, t_u, sel_d, t_d, picked, rem,
):
    comps, rows, cols = sizes
    c = lax.axis_index("comp")
    r = lax.axis_index("rows")
    k = lax.axis_index("cols")
    nf, al, ax, ln = av.shape
    ol, ox = ov.shape[1], ov.shape[2]
    nb = dsrc.shape[1]
    group = 2 * nf
    ent = nb * group
    total = comps * rows
    g = c * rows + r

    pairs = ((usrc_h, usrc), (udst_h, udst), (dsrc_h, dsrc), (drow_h, drow), (dblk_h, dblk))
    tables = [
        pltpu.make_async_copy(a, b, in_sem.at[5 + i]) for i, (a, b) in enumerate(pairs)
    ]
    ins = [
        pltpu.make_async_copy(oce, ov, in_sem.at[0]),
        pltpu.make_async_copy(atm, av, in_sem.at[1]),
        pltpu.make_async_copy(coup, cv, in_sem.at[2]),
        pltpu.make_async_copy(uw.at[0], uwv, in_sem.at[3]),
        pltpu.make_async_copy(dw.at[0], dwv, in_sem.at[4]),
    ]
    for copy in ins[:2] + tables + ins[2:]:
        copy.start()

    def x_neighbour(step):
        other = lax.rem(g + step + total, total)
        return {"comp": other // rows, "rows": lax.rem(other, rows)}

    def y_neighbour(step):
        return {"cols": lax.rem(k + step + cols, cols)}

    def row_peer(step):
        return {"rows": r ^ step}

    partners = [x_neighbour(-1), x_neighbour(1), y_neighbour(-1), y_neighbour(1)]
    partners += [row_peer(d) for d in range(1, rows)]
    barrier = pltpu.get_barrier_semaphore()
    for who in partners:
        pl.semaphore_signal(barrier, inc=1, device_id=who, device_id_type=MESH)

    lane = iota((1, ln), 1)

    ins[0].wait()
    west = jnp.zeros((ox, ln), F32)
    east = jnp.zeros((ox, ln), F32)
    for f in range(nf):
        for l in range(ol):
            q = f * ol + l
            tile = ov[f, l]
            oxs[0, q : q + 1, :] = tile[0:1, :]
            oxs[1, q : q + 1, :] = tile[ox - 1 : ox, :]
            west = jnp.where(lane == q, tile[:, 0:1], west)
            east = jnp.where(lane == q, tile[:, ln - 1 : ln], east)
    oys[0] = west
    oys[1] = east

    pl.semaphore_wait(barrier, len(partners))

    def send(src, dst, s_sem, r_sem, who):
        copy = pltpu.make_async_remote_copy(
            src_ref=src, dst_ref=dst, send_sem=s_sem, recv_sem=r_sem,
            device_id=who, device_id_type=MESH,
        )
        copy.start()
        return copy

    def exchange(which, src, dst, neighbour):
        return [
            send(src.at[i], dst.at[i], halo_s.at[which, i], halo_r.at[which, i], neighbour(step))
            for i, step in enumerate((-1, 1))
        ]

    order = range(rows - 1, 0, -1)
    surface = [
        send(ov.at[:, 0], land.at[d], land_s.at[d], land_r.at[d], row_peer(d)) for d in order
    ]
    sea_y = exchange(1, oys, oyr, y_neighbour)
    land[0] = ov[:, 0]

    second = gll_second() * VISCOSITY

    def coefficient(position, d):
        out = jnp.zeros(position.shape, F32)
        for i in range(NP):
            if 0 <= i + d < NP:
                out = jnp.where(position == i, float(second[i, i + d]), out)
        return out

    px = iota((8, ln), 0) & (NP - 1)
    py = iota((8, ln), 1) & (NP - 1)
    here = 1.0 + coefficient(px, 0) + coefficient(py, 0)
    steps = [d for d in range(1 - NP, NP) if d]
    cx = {d: coefficient(px, d) for d in steps}
    cy = {d: coefficient(py, d) for d in steps}
    ins[1].wait()
    for f in range(nf):
        for l in range(al):
            q = f * al + l
            for t in range(ax // 8):
                a = av[f, l, 8 * t : 8 * t + 8, :]
                u = here * a
                for d in steps:
                    u += cx[d] * pltpu.roll(a, (-d) % 8, 0)
                    u += cy[d] * pltpu.roll(a, (-d) % ln, 1)
                ub[q, 8 * t : 8 * t + 8, :] = u
                if t == 0:
                    axs[0, q : q + 1, :] = u[0:1, :]
                if t == ax // 8 - 1:
                    axs[1, q : q + 1, :] = u[7:8, :]

    for copy in tables:
        copy.wait()
    def column(ref):
        row = ref[...].astype(F32)
        pick = (iota((ent, nb), 0) >> bits(group)) == iota((ent, nb), 1)
        return jnp.sum(jnp.where(pick, row, 0.0), axis=1, keepdims=True)

    def spread(ref):
        row = ref[...].astype(F32)
        pick = iota((nb, nb), 0) == iota((nb, nb), 1)
        col = jnp.sum(jnp.where(pick, row, 0.0), axis=1, keepdims=True)
        pick = (iota((nb, ent), 1) >> bits(group)) == iota((nb, ent), 0)
        return jnp.sum(jnp.where(pick, col, 0.0), axis=0, keepdims=True)

    def hot(a, b):
        return jnp.where(a == b, 1.0, 0.0).astype(BF16)

    part = iota((ent, 1), 0) & (group - 1)
    part_field = (part & (nf - 1)).astype(F32)
    part_low = (part >> bits(nf)).astype(F32)
    lane_field = (iota((1, ent), 1) & (nf - 1)).astype(F32)

    s = column(usrc)
    owner = jnp.floor(s * (1.0 / ox))
    slot = (owner.astype(jnp.int32) ^ r).astype(F32)
    key = ((part_low * rows + slot) * nf + part_field) * ox + (s - owner * ox)
    sel_u[...] = hot(key, iota(sel_u.shape, 1).astype(F32))
    t_u[...] = hot(iota(t_u.shape, 0).astype(F32), lane_field * ax + spread(udst))
    key = (part_low * nf + part_field) * ax + column(dsrc)
    sel_d[...] = hot(key, iota(sel_d.shape, 1).astype(F32))
    slot = (spread(drow).astype(jnp.int32) ^ r).astype(F32)
    key = (slot * nf + lane_field) * ox + spread(dblk)
    t_d[...] = hot(iota(t_d.shape, 0).astype(F32), key)

    def remap(sel, source, weights, place):
        hi, lo = split(source)
        picked[...] = dot(sel[...], jnp.concatenate([hi, lo], axis=0))
        for b in range(nb):
            rows_b = slice(b * group, (b + 1) * group)
            rem[rows_b, :] = dot_t(picked[rows_b, :].astype(BF16), weights[b])
        hi, lo = split(rem[...])
        both = dot(place[...], jnp.concatenate([hi, lo], axis=1))
        return both[:, :ln] + both[:, ln:]

    ins[2].wait()
    ins[3].wait()
    for copy in surface:
        copy.wait_recv()
    atm_x = exchange(2, axs, axr, x_neighbour)
    sea_x = exchange(0, oxs, oxr, x_neighbour)
    sea = remap(sel_u, land[...].reshape(rows * nf * ox, ln), uwv, t_u)
    flux = cv[...] * (sea.reshape(nf, ax, ln) - av[:, al - 1])
    flb[...] = flux
    for f in range(nf):
        fxs[0, f : f + 1, :] = flb[f, 0:1, :]
        fxs[1, f : f + 1, :] = flb[f, ax - 1 : ax, :]
    flux_x = exchange(4, fxs, fxr, x_neighbour)

    ins[4].wait()
    down = remap(sel_d, flb[...].reshape(nf * ax, ln), dwv, t_d)
    dns[...] = down.reshape(rows, nf, ox, ln)
    going = [send(dns.at[d], dnr.at[d], dn_s.at[d], dn_r.at[d], row_peer(d)) for d in order]

    row_id = iota((ax, ln), 0)
    lane_id = iota((ax, ln), 1)
    first_row, last_row = row_id == 0, row_id == ax - 1
    first_lane, last_lane = lane_id == 0, lane_id == ln - 1
    x_pos, y_pos = row_id & (NP - 1), lane_id & (NP - 1)

    def average(u, axis, before, after):
        first, last, pos = (
            (first_row, last_row, x_pos) if axis == 0 else (first_lane, last_lane, y_pos)
        )
        low = jnp.where(first, before, pltpu.roll(u, 1, axis))
        high = jnp.where(last, after, pltpu.roll(u, u.shape[axis] - 1, axis))
        return jnp.where(
            pos == 0, (u + low) * 0.5, jnp.where(pos == NP - 1, (u + high) * 0.5, u)
        )

    def x_pass(copies, recv, store, packed, count):
        for copy in copies:
            copy.wait_recv()
        west = jnp.zeros((ax, ln), F32)
        east = jnp.zeros((ax, ln), F32)
        for q in range(count):
            e = average(store[q], 0, recv[1, q : q + 1, :], recv[0, q : q + 1, :])
            store[q] = e
            west = jnp.where(lane == q, e[:, 0:1], west)
            east = jnp.where(lane == q, e[:, ln - 1 : ln], east)
        packed[0] = west
        packed[1] = east

    x_pass(atm_x, axr, ub, ays, nf * al)
    atm_y = exchange(3, ays, ayr, y_neighbour)

    for copy in sea_x + sea_y:
        copy.wait_recv()
    o_row = iota((ox, ln), 0)
    o_lane = iota((ox, ln), 1)
    west = jnp.where(k == 0, 0.0, oyr[1])
    east = jnp.where(k == cols - 1, 0.0, oyr[0])

    def stencil(f, l):
        q = f * ol + l
        x = ov[f, l]
        before = jnp.where(g == 0, 0.0, oxr[1, q : q + 1, :])
        after = jnp.where(g == total - 1, 0.0, oxr[0, q : q + 1, :])
        ring = jnp.where(o_row == 0, before, pltpu.roll(x, 1, 0))
        ring += jnp.where(o_row == ox - 1, after, pltpu.roll(x, ox - 1, 0))
        ring += jnp.where(o_lane == 0, west[:, q : q + 1], pltpu.roll(x, 1, 1))
        ring += jnp.where(o_lane == ln - 1, east[:, q : q + 1], pltpu.roll(x, ln - 1, 1))
        oov[f, l] = x + DIFFUSION * (ring - 4.0 * x)

    for f in range(nf):
        for l in range(ol):
            stencil(f, l)

    x_pass(flux_x, fxr, flb, fys, nf)
    flux_y = exchange(5, fys, fyr, y_neighbour)

    for copy in atm_y:
        copy.wait_recv()
    before, after = ayr[1], ayr[0]
    for f in range(nf):
        for l in range(al):
            q = f * al + l
            aov[f, l] = average(ub[q], 1, before[:, q : q + 1], after[:, q : q + 1])

    for copy in flux_y:
        copy.wait_recv()
    before, after = fyr[1], fyr[0]
    for f in range(nf):
        e = average(flb[f], 1, before[:, f : f + 1], after[:, f : f + 1])
        aov[f, al - 1] = aov[f, al - 1] + ATM_GAIN * e

    for copy in going:
        copy.wait_recv()
    arrived = dns[0]
    for d in range(1, rows):
        arrived += dnr[d]
    oov[:, 0] = oov[:, 0] + SEA_GAIN * arrived

    for copy in surface + sea_x + sea_y + atm_x + atm_y + flux_x + flux_y + going:
        copy.wait_send()


def write_out(a, o, a_out, o_out, sem):
    copies = [
        pltpu.make_async_copy(a, a_out, sem.at[0]),
        pltpu.make_async_copy(o, o_out, sem.at[1]),
    ]
    for copy in copies:
        copy.start()
    for copy in copies:
        copy.wait()


def body(sizes, atm, oce, coup, dw, dsrc, drow, dblk, uw, udst, usrc):
    rows = sizes[1]
    nf, al, ax, ln = atm.shape
    ol, ox = oce.shape[1], oce.shape[2]
    nb, blk = dw.shape[1], dw.shape[2]
    assert ln == blk and oce.shape[3] == blk
    fa, fo, ent = nf * al, nf * ol, nb * 2 * nf
    assert fa <= ln and fo <= ln
    vm = pltpu.VMEM
    dma = pltpu.SemaphoreType.DMA
    pair = lambda n: [vm((2, n, ln), F32)] * 2
    scratch = [
        vm(atm.shape, F32), vm(oce.shape, F32), vm(coup.shape, F32),
        vm((nb, blk, blk), BF16), vm((nb, blk, blk), BF16), dma((10,)),
        *([vm(dsrc.shape, jnp.int32)] * 5),
        vm((rows, nf, ox, ln), F32), dma((rows,)), dma((rows,)),
        *pair(fo), *pair(ox), *pair(fa), *pair(ax), *pair(nf), *pair(ax),
        dma((6, 2)), dma((6, 2)),
        vm((rows, nf, ox, ln), F32), vm((rows, nf, ox, ln), F32), dma((rows,)), dma((rows,)),
        vm((fa, ax, ln), F32), vm((nf, ax, ln), F32),
        vm((ent, 2 * rows * nf * ox), BF16), vm((nf * ax, ent), BF16),
        vm((ent, 2 * nf * ax), BF16), vm((rows * nf * ox, ent), BF16),
        vm((ent, ln), F32), vm((ent, ln), F32),
    ]
    args = (atm, oce, coup, dw, dsrc, drow, dblk, uw, udst, usrc)
    args = [pltpu.with_memory_space_constraint(x, pltpu.HBM) for x in args]
    hbm = pl.BlockSpec(memory_space=pltpu.HBM)
    small = pl.BlockSpec(memory_space=pltpu.VMEM)
    held = pl.pallas_call(
        functools.partial(kernel, sizes),
        out_shape=(
            jax.ShapeDtypeStruct(atm.shape, F32),
            jax.ShapeDtypeStruct(oce.shape, F32),
        ),
        in_specs=[hbm] * len(args),
        out_specs=(small, small),
        scratch_shapes=scratch,
        compiler_params=pltpu.CompilerParams(collective_id=0, has_side_effects=True, vmem_limit_bytes=24 << 20
        ),
        name="coupled_step",
    )(*args)
    return pl.pallas_call(
        write_out,
        out_shape=(jax.ShapeDtypeStruct(atm.shape, F32), jax.ShapeDtypeStruct(oce.shape, F32)),
        in_specs=[small, small],
        out_specs=(hbm, hbm),
        scratch_shapes=[dma((2,))],
        compiler_params=pltpu.CompilerParams(vmem_limit_bytes=8 << 20),
        name="write_out",
    )(*held)


def solution(mesh):
    sizes = tuple(mesh.shape[a] for a in ("comp", "rows", "cols"))
    tiles = P(None, None, ("comp", "rows"), "cols")
    flat = P(("comp", "rows"), "cols")
    blocks = P(("comp", "rows"), "cols", None, None)
    return jax.shard_map(
        functools.partial(body, sizes),
        mesh=mesh,
        in_specs=(tiles, tiles, flat, blocks, flat, flat, flat, blocks, flat, flat),
        out_specs=(tiles, tiles),
        check_vma=False,
    )
```

```python
import functools

import jax
import jax.numpy as jnp
import numpy as np
from jax import lax
from jax.experimental import pallas as pl
from jax.experimental.pallas import tpu as pltpu
from jax.sharding import PartitionSpec as P

NP = 4
VISCOSITY = 0.01
ATM_GAIN = 0.5
DIFFUSION = 0.1
SEA_GAIN = 0.5
MESH = pl.DeviceIdType.MESH
F32 = jnp.float32
BF16 = jnp.bfloat16


def gll_second():
    gll_nodes = np.array([-1.0, -1.0 / np.sqrt(5.0), 1.0 / np.sqrt(5.0), 1.0])
    n = gll_nodes.shape[0]
    bary = np.array(
        [1.0 / np.prod([gll_nodes[c] - gll_nodes[o] for o in range(n) if o != c]) for c in range(n)]
    )
    derivative = np.zeros((n, n))
    for r in range(n):
        for c in range(n):
            if r != c:
                derivative[r, c] = bary[c] / bary[r] / (gll_nodes[r] - gll_nodes[c])
        derivative[r, r] = -np.sum(derivative[r])
    return derivative @ derivative


def iota(shape, dim):
    return lax.broadcasted_iota(jnp.int32, shape, dim)


def bits(n):
    assert n & (n - 1) == 0
    return n.bit_length() - 1


def split(x):
    hi = x.astype(BF16)
    return hi, (x - hi.astype(F32)).astype(BF16)


def dot(a, b):
    return jnp.dot(a, b, preferred_element_type=F32)


def dot_t(a, b):
    return lax.dot_general(a, b, (((1,), (1,)), ((), ())), preferred_element_type=F32)


def kernel(
    sizes,
    atm, oce, coup, dw, dsrc_h, drow_h, dblk_h, uw, udst_h, usrc_h,
    aov, oov,
    av, ov, cv, dwv, uwv, in_sem, usrc, udst, dsrc, drow, dblk,
    land, land_s, land_r,
    oxs, oxr, oys, oyr, axs, axr, ays, ayr, fxs, fxr, fys, fyr, halo_s, halo_r, fx_s, fx_r, relay,
    dns, dnr, dn_s, dn_r,
    ub, flb, sel_u, t_u, sel_d, t_d, picked, rem,
):
    comps, rows, cols = sizes
    c = lax.axis_index("comp")
    r = lax.axis_index("rows")
    k = lax.axis_index("cols")
    nf, al, ax, ln = av.shape
    ol, ox = ov.shape[1], ov.shape[2]
    nb = dsrc.shape[1]
    group = 2 * nf
    ent = nb * group
    total = comps * rows
    g = c * rows + r

    pairs = ((usrc_h, usrc), (udst_h, udst), (dsrc_h, dsrc), (drow_h, drow), (dblk_h, dblk))
    tables = [
        pltpu.make_async_copy(a, b, in_sem.at[5 + i]) for i, (a, b) in enumerate(pairs)
    ]
    ins = [
        pltpu.make_async_copy(oce, ov, in_sem.at[0]),
        pltpu.make_async_copy(atm, av, in_sem.at[1]),
        pltpu.make_async_copy(coup, cv, in_sem.at[2]),
        pltpu.make_async_copy(uw.at[0], uwv, in_sem.at[3]),
        pltpu.make_async_copy(dw.at[0], dwv, in_sem.at[4]),
    ]
    for copy in ins[:2] + tables + ins[2:]:
        copy.start()

    def x_neighbour(step):
        other = lax.rem(g + step + total, total)
        return {"comp": other // rows, "rows": lax.rem(other, rows)}

    def y_neighbour(step):
        return {"cols": lax.rem(k + step + cols, cols)}

    def corner(step, side):
        return {**x_neighbour(step), **y_neighbour(side)}

    def row_peer(step):
        return {"rows": r ^ step}

    def comp_neighbour(step):
        return {"comp": lax.rem(c + step + comps, comps)}

    across = [comp_neighbour(-1), comp_neighbour(1)] if comps > 1 else []
    partners = [y_neighbour(-1), y_neighbour(1)] + across
    partners += [row_peer(d) for d in range(1, rows)]
    barrier = pltpu.get_barrier_semaphore()
    for who in partners:
        pl.semaphore_signal(barrier, inc=1, device_id=who, device_id_type=MESH)

    lane = iota((1, ln), 1)

    ins[0].wait()
    west = jnp.zeros((ox, ln), F32)
    east = jnp.zeros((ox, ln), F32)
    for f in range(nf):
        for l in range(ol):
            q = f * ol + l
            tile = ov[f, l]
            oxs[0, q : q + 1, :] = tile[0:1, :]
            oxs[1, q : q + 1, :] = tile[ox - 1 : ox, :]
            west = jnp.where(lane == q, tile[:, 0:1], west)
            east = jnp.where(lane == q, tile[:, ln - 1 : ln], east)
    oys[0] = west
    oys[1] = east

    pl.semaphore_wait(barrier, len(partners))

    def send(src, dst, s_sem, r_sem, who):
        copy = pltpu.make_async_remote_copy(
            src_ref=src, dst_ref=dst, send_sem=s_sem, recv_sem=r_sem,
            device_id=who, device_id_type=MESH,
        )
        copy.start()
        return copy

    def exchange(which, src, dst, neighbour):
        return [
            send(src.at[i], dst.at[i], halo_s.at[which, i], halo_r.at[which, i], neighbour(step))
            for i, step in enumerate((-1, 1))
        ]

    order = range(rows - 1, 0, -1)
    surface = [
        send(ov.at[:, 0], land.at[d], land_s.at[d], land_r.at[d], row_peer(d)) for d in order
    ]
    for who in across:
        pl.semaphore_signal(relay, inc=1, device_id=who, device_id_type=MESH)
    land[0] = ov[:, 0]

    second = gll_second() * VISCOSITY

    def coefficient(position, d):
        out = jnp.zeros(position.shape, F32)
        for i in range(NP):
            if 0 <= i + d < NP:
                out = jnp.where(position == i, float(second[i, i + d]), out)
        return out

    px = iota((8, ln), 0) & (NP - 1)
    py = iota((8, ln), 1) & (NP - 1)
    here = 1.0 + coefficient(px, 0) + coefficient(py, 0)
    steps = [d for d in range(1 - NP, NP) if d]
    cx = {d: coefficient(px, d) for d in steps}
    cy = {d: coefficient(py, d) for d in steps}
    ins[1].wait()
    for f in range(nf):
        for l in range(al):
            q = f * al + l
            for t in range(ax // 8):
                a = av[f, l, 8 * t : 8 * t + 8, :]
                u = here * a
                for d in steps:
                    u += cx[d] * pltpu.roll(a, (-d) % 8, 0)
                    u += cy[d] * pltpu.roll(a, (-d) % ln, 1)
                ub[q, 8 * t : 8 * t + 8, :] = u
                if t == 0:
                    axs[0, q : q + 1, :] = u[0:1, :]
                if t == ax // 8 - 1:
                    axs[1, q : q + 1, :] = u[7:8, :]

    if across:
        pl.semaphore_wait(relay, len(across))
    sea_y = exchange(1, oys, oyr, y_neighbour)
    atm_x = exchange(2, axs, axr, x_neighbour)

    for copy in tables:
        copy.wait()
    def column(ref):
        row = ref[...].astype(F32)
        pick = (iota((ent, nb), 0) >> bits(group)) == iota((ent, nb), 1)
        return jnp.sum(jnp.where(pick, row, 0.0), axis=1, keepdims=True)

    def spread(ref):
        row = ref[...].astype(F32)
        pick = iota((nb, nb), 0) == iota((nb, nb), 1)
        col = jnp.sum(jnp.where(pick, row, 0.0), axis=1, keepdims=True)
        pick = (iota((nb, ent), 1) >> bits(group)) == iota((nb, ent), 0)
        return jnp.sum(jnp.where(pick, col, 0.0), axis=0, keepdims=True)

    def hot(a, b):
        return jnp.where(a == b, 1.0, 0.0).astype(BF16)

    part = iota((ent, 1), 0) & (group - 1)
    part_field = (part & (nf - 1)).astype(F32)
    part_low = (part >> bits(nf)).astype(F32)
    lane_field = (iota((1, ent), 1) & (nf - 1)).astype(F32)

    s = column(usrc)
    owner = jnp.floor(s * (1.0 / ox))
    slot = (owner.astype(jnp.int32) ^ r).astype(F32)
    key = ((part_low * rows + slot) * nf + part_field) * ox + (s - owner * ox)
    sel_u[...] = hot(key, iota(sel_u.shape, 1).astype(F32))
    t_u[...] = hot(iota(t_u.shape, 0).astype(F32), lane_field * ax + spread(udst))
    key = (part_low * nf + part_field) * ax + column(dsrc)
    sel_d[...] = hot(key, iota(sel_d.shape, 1).astype(F32))
    slot = (spread(drow).astype(jnp.int32) ^ r).astype(F32)
    key = (slot * nf + lane_field) * ox + spread(dblk)
    t_d[...] = hot(iota(t_d.shape, 0).astype(F32), key)

    def remap(sel, source, weights, place):
        hi, lo = split(source)
        picked[...] = dot(sel[...], jnp.concatenate([hi, lo], axis=0))
        for b in range(nb):
            rows_b = slice(b * group, (b + 1) * group)
            rem[rows_b, :] = dot_t(picked[rows_b, :].astype(BF16), weights[b])
        hi, lo = split(rem[...])
        both = dot(place[...], jnp.concatenate([hi, lo], axis=1))
        return both[:, :ln] + both[:, ln:]

    ins[2].wait()
    ins[3].wait()
    for copy in surface + sea_y:
        copy.wait_recv()
    sea_x = exchange(0, oxs, oxr, x_neighbour)
    sea = remap(sel_u, land[...].reshape(rows * nf * ox, ln), uwv, t_u)
    flux = cv[...] * (sea.reshape(nf, ax, ln) - av[:, al - 1])
    flb[...] = flux
    west = jnp.zeros((ax, ln), F32)
    east = jnp.zeros((ax, ln), F32)
    for f in range(nf):
        e = flux[f]
        fxs[0, f : f + 1, :] = e[0:1, :]
        fxs[1, f : f + 1, :] = e[ax - 1 : ax, :]
        west = jnp.where(lane == f, e[:, 0:1], west)
        east = jnp.where(lane == f, e[:, ln - 1 : ln], east)
    fys[0] = west
    fys[1] = east
    flux_x = [
        send(fxs.at[i], fxr.at[i, j], fx_s.at[i, j], fx_r.at[i, j], corner(step, side))
        for i, step in enumerate((-1, 1))
        for j, side in enumerate((-1, 0, 1))
    ]
    flux_y = exchange(4, fys, fyr, y_neighbour)

    ins[4].wait()
    down = remap(sel_d, flb[...].reshape(nf * ax, ln), dwv, t_d)
    dns[...] = down.reshape(rows, nf, ox, ln)
    going = [send(dns.at[d], dnr.at[d], dn_s.at[d], dn_r.at[d], row_peer(d)) for d in order]

    row_id = iota((ax, ln), 0)
    lane_id = iota((ax, ln), 1)
    first_row, last_row = row_id == 0, row_id == ax - 1
    first_lane, last_lane = lane_id == 0, lane_id == ln - 1
    x_pos, y_pos = row_id & (NP - 1), lane_id & (NP - 1)

    def average(u, axis, before, after):
        first, last, pos = (
            (first_row, last_row, x_pos) if axis == 0 else (first_lane, last_lane, y_pos)
        )
        low = jnp.where(first, before, pltpu.roll(u, 1, axis))
        high = jnp.where(last, after, pltpu.roll(u, u.shape[axis] - 1, axis))
        return jnp.where(
            pos == 0, (u + low) * 0.5, jnp.where(pos == NP - 1, (u + high) * 0.5, u)
        )

    def x_pass(copies, recv, store, packed, count):
        for copy in copies:
            copy.wait_recv()
        west = jnp.zeros((ax, ln), F32)
        east = jnp.zeros((ax, ln), F32)
        for q in range(count):
            e = average(store[q], 0, recv[1, q : q + 1, :], recv[0, q : q + 1, :])
            store[q] = e
            west = jnp.where(lane == q, e[:, 0:1], west)
            east = jnp.where(lane == q, e[:, ln - 1 : ln], east)
        packed[0] = west
        packed[1] = east

    x_pass(atm_x, axr, ub, ays, nf * al)
    atm_y = exchange(3, ays, ayr, y_neighbour)

    for copy in sea_x:
        copy.wait_recv()
    o_row = iota((ox, ln), 0)
    o_lane = iota((ox, ln), 1)
    west = jnp.where(k == 0, 0.0, oyr[1])
    east = jnp.where(k == cols - 1, 0.0, oyr[0])

    def stencil(f, l):
        q = f * ol + l
        x = ov[f, l]
        before = jnp.where(g == 0, 0.0, oxr[1, q : q + 1, :])
        after = jnp.where(g == total - 1, 0.0, oxr[0, q : q + 1, :])
        ring = jnp.where(o_row == 0, before, pltpu.roll(x, 1, 0))
        ring += jnp.where(o_row == ox - 1, after, pltpu.roll(x, ox - 1, 0))
        ring += jnp.where(o_lane == 0, west[:, q : q + 1], pltpu.roll(x, 1, 1))
        ring += jnp.where(o_lane == ln - 1, east[:, q : q + 1], pltpu.roll(x, ln - 1, 1))
        oov[f, l] = x + DIFFUSION * (ring - 4.0 * x)

    for f in range(nf):
        for l in range(ol):
            stencil(f, l)

    for copy in atm_y:
        copy.wait_recv()
    before, after = ayr[1], ayr[0]
    for f in range(nf):
        for l in range(al):
            q = f * al + l
            aov[f, l] = average(ub[q], 1, before[:, q : q + 1], after[:, q : q + 1])

    for copy in flux_x + flux_y:
        copy.wait_recv()

    def corners(i, j, at):
        row = jnp.zeros((1, ln), F32)
        for f in range(nf):
            row = jnp.where(lane == f, fxr[i, j, f : f + 1, at : at + 1], row)
        return row

    before = average(fyr[1], 0, corners(1, 2, ln - 1), corners(0, 2, ln - 1))
    after = average(fyr[0], 0, corners(1, 0, 0), corners(0, 0, 0))
    for f in range(nf):
        e = average(flb[f], 0, fxr[1, 1, f : f + 1, :], fxr[0, 1, f : f + 1, :])
        e = average(e, 1, before[:, f : f + 1], after[:, f : f + 1])
        aov[f, al - 1] = aov[f, al - 1] + ATM_GAIN * e

    for copy in going:
        copy.wait_recv()
    arrived = dns[0]
    for d in range(1, rows):
        arrived += dnr[d]
    oov[:, 0] = oov[:, 0] + SEA_GAIN * arrived

    for copy in surface + sea_x + sea_y + atm_x + atm_y + flux_x + flux_y + going:
        copy.wait_send()


def write_out(a, o, a_out, o_out, sem):
    copies = [
        pltpu.make_async_copy(a, a_out, sem.at[0]),
        pltpu.make_async_copy(o, o_out, sem.at[1]),
    ]
    for copy in copies:
        copy.start()
    for copy in copies:
        copy.wait()


def body(sizes, atm, oce, coup, dw, dsrc, drow, dblk, uw, udst, usrc):
    rows = sizes[1]
    nf, al, ax, ln = atm.shape
    ol, ox = oce.shape[1], oce.shape[2]
    nb, blk = dw.shape[1], dw.shape[2]
    assert ln == blk and oce.shape[3] == blk
    fa, fo, ent = nf * al, nf * ol, nb * 2 * nf
    assert fa <= ln and fo <= ln
    vm = pltpu.VMEM
    dma = pltpu.SemaphoreType.DMA
    pair = lambda n: [vm((2, n, ln), F32)] * 2
    scratch = [
        vm(atm.shape, F32), vm(oce.shape, F32), vm(coup.shape, F32),
        vm((nb, blk, blk), BF16), vm((nb, blk, blk), BF16), dma((10,)),
        *([vm(dsrc.shape, jnp.int32)] * 5),
        vm((rows, nf, ox, ln), F32), dma((rows,)), dma((rows,)),
        *pair(fo), *pair(ox), *pair(fa), *pair(ax),
        vm((2, nf, ln), F32), vm((2, 3, nf, ln), F32), *pair(ax),
        dma((5, 2)), dma((5, 2)), dma((2, 3)), dma((2, 3)),
        pltpu.SemaphoreType.REGULAR,
        vm((rows, nf, ox, ln), F32), vm((rows, nf, ox, ln), F32), dma((rows,)), dma((rows,)),
        vm((fa, ax, ln), F32), vm((nf, ax, ln), F32),
        vm((ent, 2 * rows * nf * ox), BF16), vm((nf * ax, ent), BF16),
        vm((ent, 2 * nf * ax), BF16), vm((rows * nf * ox, ent), BF16),
        vm((ent, ln), F32), vm((ent, ln), F32),
    ]
    args = (atm, oce, coup, dw, dsrc, drow, dblk, uw, udst, usrc)
    args = [pltpu.with_memory_space_constraint(x, pltpu.HBM) for x in args]
    hbm = pl.BlockSpec(memory_space=pltpu.HBM)
    small = pl.BlockSpec(memory_space=pltpu.VMEM)
    held = pl.pallas_call(
        functools.partial(kernel, sizes),
        out_shape=(
            jax.ShapeDtypeStruct(atm.shape, F32),
            jax.ShapeDtypeStruct(oce.shape, F32),
        ),
        in_specs=[hbm] * len(args),
        out_specs=(small, small),
        scratch_shapes=scratch,
        compiler_params=pltpu.CompilerParams(collective_id=0, has_side_effects=True, vmem_limit_bytes=24 << 20
        ),
        name="coupled_step",
    )(*args)
    return pl.pallas_call(
        write_out,
        out_shape=(jax.ShapeDtypeStruct(atm.shape, F32), jax.ShapeDtypeStruct(oce.shape, F32)),
        in_specs=[small, small],
        out_specs=(hbm, hbm),
        scratch_shapes=[dma((2,))],
        compiler_params=pltpu.CompilerParams(vmem_limit_bytes=8 << 20),
        name="write_out",
    )(*held)


def solution(mesh):
    sizes = tuple(mesh.shape[a] for a in ("comp", "rows", "cols"))
    tiles = P(None, None, ("comp", "rows"), "cols")
    flat = P(("comp", "rows"), "cols")
    blocks = P(("comp", "rows"), "cols", None, None)
    return jax.shard_map(
        functools.partial(body, sizes),
        mesh=mesh,
        in_specs=(tiles, tiles, flat, blocks, flat, flat, flat, blocks, flat, flat),
        out_specs=(tiles, tiles),
        check_vma=False,
    )
```
